32 devices in a mesh: rows: 8 (over y, x, core), cores: 4 (over z).
Axes of the slice: x: 2, y: 2, z: 4, core: 2. Of those that a mesh axis runs over, the one named last changes fastest.
Arguments:
- rhs: float32 [131072, 128], P(('rows', 'cores')), may hold values from -6 to 6
- guess: float32 [131072, 128], P(('rows', 'cores')), may hold values from -4 to 4
- degree: float32 [131072], P(('rows', 'cores')), may hold values from 2 to 6
- weights: bfloat16 [1024, 16, 128, 128], P(('rows', 'cores')), may hold values from -0.1875 to 0.1875
- columns: int32 [1024, 16], P(('rows', 'cores')), may hold values from 0 to 95, as said below
- block_counts: int32 [1024], P(('rows', 'cores')), may hold values from 8 to 16, as said below
- send_lists: int32 [32, 32, 2], P(('rows', 'cores')), may hold values from 0 to 31
- aggregates: int32 [131072], P(('rows', 'cores')), may hold values from 0 to 16383
- coarse_diag: float32 [16384], replicated, may hold values from 4 to 32
Outputs:
- smoothed: float32 [131072, 128], P(('rows', 'cores'))
The draws below stay inside these ranges and needn't reach their ends.
Inputs may be any that keep to these rules, and one draw needn't show every extreme that they name: `block_counts`: every block row has 8 or 16 live slots, and the rows of one device have exactly 320 live slots in all. `columns`: on every device, each table index from 32 up is named by at least one live slot.
All inputs are finite; a program needn't handle non-finite values.
Results may differ from the reference program's by a relative error of at most 0.0022.
Values may be sent and summed in bfloat16 or wider, within the bound.
No kernel may reach another device: no remote copies, remote signals or barrier semaphores. Data moves between devices by JAX's collectives and lax.ppermute only.
A program may use at most 128 MiB of HBM per device.

```python
import math
import jax
import jax.numpy as jnp
from jax import lax

NB_DEV = 32
BLOCK = 128
SLOTS = 16
MAXB = 2
RHS = 128
NC = 16384
NBLK = 1024
NV = 131072
DEVICES = 32


def counts_table(key):
    base = jax.random.fold_in(key, 11)
    keys = jax.random.split(base, DEVICES)
    perms = jax.vmap(lambda single: jax.random.permutation(single, NB_DEV))(keys)
    hubby = perms < NB_DEV // 4
    return jnp.where(hubby, SLOTS, SLOTS // 2).astype(jnp.int32)


def draw_block_counts(key, part):
    return counts_table(key).reshape(-1)


def draw_columns(key, part):
    counts = counts_table(key)
    live = (jnp.arange(SLOTS, dtype=jnp.int32)[None, None, :] < counts[:, :, None]).reshape(DEVICES, -1).astype(jnp.int32)
    ranks = jnp.cumsum(live, axis=1) - 1
    remote = DEVICES * MAXB
    livecount = NB_DEV * SLOTS * 5 // 8
    keys = jax.random.split(jax.random.fold_in(key, 23), DEVICES)
    perms = jax.vmap(lambda single: jax.random.permutation(single, livecount))(keys).astype(jnp.int32)
    assigned = jnp.take_along_axis(perms, jnp.clip(ranks, 0, livecount - 1), axis=1)
    filler = jax.random.randint(jax.random.fold_in(key, 31), live.shape, 0, NB_DEV + remote)
    chosen = jnp.where((live == 1) & (assigned < remote), NB_DEV + assigned, filler)
    return chosen.reshape(NB_DEV * DEVICES, SLOTS).astype(jnp.int32)


def draw_aggregates(key, part):
    total = NB_DEV * DEVICES * BLOCK
    per_owner = NC // DEVICES
    device = jnp.arange(total, dtype=jnp.int32) // (NB_DEV * BLOCK)
    inside = jax.random.randint(jax.random.fold_in(key, 41), (total,), 0, per_owner)
    anywhere = jax.random.randint(jax.random.fold_in(key, 47), (total,), 0, NC)
    across = jax.random.randint(jax.random.fold_in(key, 43), (total,), 0, 2) == 0
    own = device * per_owner + inside
    return jnp.where(across, anywhere, own).astype(jnp.int32)


def touch_ends(drawn, rng, low, top_value):
    dims = drawn.shape
    index_at = [jax.random.randint(jax.random.fold_in(rng, axis), (), 0, dims[axis]) for axis in range(len(dims))]
    drawn = drawn.at[tuple(index_at)].set(low)
    longest = dims.index(max(dims))
    index_at[longest] = (index_at[longest] + 1) % dims[longest]
    return drawn.at[tuple(index_at)].set(top_value)


def block_levels(rng, shape, shards, least, high):
    def one(axis_at, shards_of):
        steps = jax.random.uniform(jax.random.fold_in(jax.random.fold_in(rng, 6), axis_at), (shards_of,), jnp.float32, least / len(shards), high / len(shards))
        return jnp.repeat(jnp.exp(steps), shape[axis_at] // shards_of).reshape((-1,) + (1,) * (len(shape) - axis_at - 1))

    loudness = one(*shards[0])
    for cut in shards[1:]:
        loudness = loudness * one(*cut)
    return loudness


def bell_draw(own_key, shape, deviation, bound, shards=(), held_as=jnp.bfloat16):
    level = block_levels(own_key, shape, shards, -0.22, 0.18) if shards else 1.0
    drawn = jax.random.normal(own_key, shape, jnp.float32) * deviation * level
    return jnp.minimum(jnp.maximum(drawn, -bound), bound).astype(held_as)


def setup_inputs(seed: int = 0) -> dict:
    key_of = jax.random.split(jax.random.key(seed), 10)
    return {
        "rhs": bell_draw(key_of[0], (NV, RHS), 1.0, 6.0, ((0, 32),), jnp.float32),
        "guess": bell_draw(key_of[1], (NV, RHS), 0.5, 4.0, ((0, 32),), jnp.float32),
        "degree": jnp.clip(jnp.exp(math.log(6.0) - 1.0986123 * jax.random.uniform(key_of[2], (NV,), jnp.float32) ** block_levels(key_of[2], (NV,), ((0, 32),), -0.2, 0.2)), 2.0, 6.0),
        "weights": bell_draw(key_of[3], (NBLK, SLOTS, BLOCK, BLOCK), (BLOCK * 8) ** -0.5, 0.1875, ((0, 32),)),
        "columns": draw_columns(jax.random.fold_in(key_of[9], 71), 0),
        "block_counts": draw_block_counts(jax.random.fold_in(key_of[9], 71), 0),
        "send_lists": touch_ends(jax.random.randint(key_of[6], (DEVICES, DEVICES, MAXB), 0, NB_DEV), jax.random.fold_in(key_of[6], 1), 0, NB_DEV - 1).astype(jnp.int32),
        "aggregates": draw_aggregates(jax.random.fold_in(key_of[9], 71), 0),
        "coarse_diag": jnp.clip(jnp.exp(jax.random.uniform(key_of[8], (NC,), jnp.float32, math.log(4.0), math.log(32.0))), 4.0, 32.0),
    }


damping = 0.7


def reference(rhs, guess, degree, weights, columns, block_counts, send_lists, aggregates, coarse_diag):
    nblk = weights.shape[0]
    live = (jnp.arange(SLOTS, dtype=jnp.int32)[None, :] < block_counts[:, None]).astype(jnp.bfloat16)
    live_weights = weights * live[:, :, None, None]

    def apply(field):
        blocks = field.astype(jnp.bfloat16).reshape(nblk, BLOCK, RHS)

        def one(device):
            local = lax.dynamic_slice_in_dim(blocks, device * NB_DEV, NB_DEV, 0)
            owners = jnp.arange(DEVICES, dtype=jnp.int32)[:, None] * NB_DEV
            wanted = (owners + send_lists[:, device, :]).reshape(-1).astype(jnp.int32)
            table = jnp.concatenate([local, blocks[wanted]], 0)
            wpart = lax.dynamic_slice_in_dim(live_weights, device * NB_DEV, NB_DEV, 0)
            cpart = lax.dynamic_slice_in_dim(columns, device * NB_DEV, NB_DEV, 0)
            return jnp.einsum('bsij,bsjr->bir', wpart.astype(jnp.float32), table[cpart].astype(jnp.float32))

        offsum = lax.map(one, jnp.arange(DEVICES, dtype=jnp.int32)).reshape(-1, RHS)
        return degree[:, None] * field - offsum

    first = guess + damping * (rhs - apply(guess)) / degree[:, None]
    residue = rhs - apply(first)
    coarse = jax.ops.segment_sum(residue, aggregates, num_segments=NC)
    correction = (coarse / coarse_diag[:, None]).astype(jnp.bfloat16)
    second = first + correction[aggregates].astype(jnp.float32)
    return second + damping * (rhs - apply(second)) / degree[:, None]
```

```python
import functools

import jax
import jax.numpy as jnp
from jax import lax
from jax.experimental import pallas as pl
from jax.experimental.pallas import tpu as pltpu
from jax.sharding import PartitionSpec as P

AXES = ("rows", "cores")
DAMPING = 0.7
VMEM_LIMIT = 60 * 1024 * 1024
HALF = 8
BATCH = 4


HBM = pl.BlockSpec(memory_space=pl.ANY)
SMEM = pl.BlockSpec(memory_space=pltpu.SMEM)


def copy(src, dst, sem):
    return pltpu.make_async_copy(src, dst, sem)


def send_blocks(lists, packed, outgoing, sem):
    @pl.loop(0, outgoing.shape[0])
    def _(i):
        copy(packed.at[lists[i]], outgoing.at[i], sem).start()


def pack_kernel(lists, field, outgoing, field_v, packed, in_sem, out_sem):
    blocks = field.shape[0]

    @pl.loop(0, blocks)
    def _(b):
        copy(field.at[b], field_v.at[b], in_sem.at[b]).start()

    @pl.loop(0, blocks)
    def _(b):
        copy(field.at[b], field_v.at[b], in_sem.at[b]).wait()
        packed[b] = field_v[b].astype(packed.dtype)

    send_blocks(lists, packed, outgoing, out_sem)
    copy(outgoing, outgoing, out_sem).wait()


def pack(lists, field):
    blocks, size, width = field.shape
    return pl.pallas_call(
        pack_kernel,
        out_shape=jax.ShapeDtypeStruct((lists.shape[0], size, width), jnp.bfloat16),
        in_specs=[SMEM, HBM],
        out_specs=HBM,
        scratch_shapes=[
            pltpu.VMEM(field.shape, field.dtype),
            pltpu.VMEM(field.shape, jnp.bfloat16),
            pltpu.SemaphoreType.DMA((blocks,)),
            pltpu.SemaphoreType.DMA,
        ],
        compiler_params=pltpu.CompilerParams(vmem_limit_bytes=VMEM_LIMIT),
        name="pack",
    )(lists, field)


def start_weights(counts, weights, weights_v, sem, b):
    for h in range(weights.shape[1] // HALF):
        half = pl.ds(h * HALF, HALF)

        @pl.when(counts[b] > h * HALF)
        def _():
            copy(weights.at[b, half], weights_v.at[b, half], sem.at[b, h]).start()


def block_product(columns, counts, weights, weights_v, table, total, sem, b):
    slots = weights.shape[1]
    for h in range(slots // HALF):
        half = pl.ds(h * HALF, HALF)

        @pl.when(counts[b] > h * HALF)
        def _():
            copy(weights.at[b, half], weights_v.at[b, half], sem.at[b, h]).wait()
            left = [weights_v[b, h * HALF + s] for s in range(HALF)]
            right = [table[columns[b * slots + h * HALF + s]] for s in range(HALF)]
            product = jnp.dot(
                jnp.concatenate(left, 1),
                jnp.concatenate(right, 0),
                preferred_element_type=jnp.float32,
            )
            if h == 0:
                total[...] = product
            else:
                total[...] += product


def load_operands(counts, weights, rows, weights_v, rows_v, weights_sem, rows_sem):
    @pl.loop(0, weights.shape[0])
    def _(b):
        start_weights(counts, weights, weights_v, weights_sem, b)
        for k, (src, dst) in enumerate(zip(rows, rows_v)):
            copy(src.at[b], dst.at[b], rows_sem.at[b, k]).start()


def wait_rows(rows, rows_v, rows_sem, b):
    for k, (src, dst) in enumerate(zip(rows, rows_v)):
        copy(src.at[b], dst.at[b], rows_sem.at[b, k]).wait()


def first_kernel(
    columns, counts, lists, weights, field, incoming, rhs, degree,
    result, outgoing,
    weights_v, table, field_v, rhs_v, degree_v, result_v, packed, total,
    weights_sem, rows_sem, field_sem, halo_sem, result_sem, out_sem,
):
    blocks = weights.shape[0]
    halo = table.at[pl.ds(blocks, incoming.shape[0])]
    copy(field, field_v, field_sem).start()
    copy(incoming, halo, halo_sem).start()
    load_operands(
        counts, weights, (rhs, degree), weights_v, (rhs_v, degree_v), weights_sem, rows_sem
    )
    copy(field, field_v, field_sem).wait()

    @pl.loop(0, blocks)
    def _(b):
        table[b] = field_v[b].astype(table.dtype)

    copy(incoming, halo, halo_sem).wait()

    @pl.loop(0, blocks)
    def _(b):
        block_product(columns, counts, weights, weights_v, table, total, weights_sem, b)
        wait_rows((rhs, degree), (rhs_v, degree_v), rows_sem, b)
        x, d = field_v[b], degree_v[b]
        first = x + DAMPING * (rhs_v[b] - (d * x - total[...])) / d
        result_v[b] = first
        packed[b] = first.astype(packed.dtype)
        copy(result_v.at[b], result.at[b], result_sem).start()

    send_blocks(lists, packed, outgoing, out_sem)
    copy(result_v, result, result_sem).wait()
    copy(outgoing, outgoing, out_sem).wait()


def first_step(columns, counts, lists, weights, field, incoming, rhs, degree):
    blocks, size, width = field.shape
    slots = weights.shape[1]
    f32, bf16 = jnp.float32, jnp.bfloat16
    return pl.pallas_call(
        first_kernel,
        out_shape=(
            jax.ShapeDtypeStruct(field.shape, f32),
            jax.ShapeDtypeStruct((lists.shape[0], size, width), bf16),
        ),
        in_specs=[SMEM] * 3 + [HBM] * 5,
        out_specs=(HBM, HBM),
        scratch_shapes=[
            pltpu.VMEM(weights.shape, bf16),
            pltpu.VMEM((blocks + incoming.shape[0], size, width), bf16),
            pltpu.VMEM(field.shape, f32),
            pltpu.VMEM(field.shape, f32),
            pltpu.VMEM(field.shape, f32),
            pltpu.VMEM(field.shape, f32),
            pltpu.VMEM(field.shape, bf16),
            pltpu.VMEM((size, width), f32),
            pltpu.SemaphoreType.DMA((blocks, slots // HALF)),
            pltpu.SemaphoreType.DMA((blocks, 2)),
            pltpu.SemaphoreType.DMA,
            pltpu.SemaphoreType.DMA,
            pltpu.SemaphoreType.DMA,
            pltpu.SemaphoreType.DMA,
        ],
        compiler_params=pltpu.CompilerParams(vmem_limit_bytes=VMEM_LIMIT),
        cost_estimate=pl.CostEstimate(
            flops=2 * blocks * slots * size * size * width,
            bytes_accessed=24 << 20, transcendentals=0,
        ),
        name="first",
    )(columns, counts, lists, weights, field, incoming, rhs, degree)


def second_kernel(
    columns, counts, targets, weights, field, incoming, rhs, degree,
    base, part0, part1, part2, part3,
    weights_v, table, field_v, rhs_v, degree_v, base_v, residue, coarse, coarse_b, total,
    weights_sem, rows_sem, field_sem, halo_sem, base_sem, part_sem,
):
    blocks, size = field.shape[0], field.shape[1]
    halo = table.at[pl.ds(blocks, incoming.shape[0])]
    copy(field, field_v, field_sem).start()
    copy(incoming, halo, halo_sem).start()
    load_operands(
        counts, weights, (rhs, degree), weights_v, (rhs_v, degree_v), weights_sem, rows_sem
    )

    aggregates = coarse.shape[0]
    chunk = 256

    @pl.loop(0, aggregates // chunk)
    def _(i):
        coarse[pl.ds(pl.multiple_of(i * chunk, chunk), chunk), :] = jnp.zeros(
            (chunk, coarse.shape[1]), jnp.float32
        )

    copy(field, field_v, field_sem).wait()

    @pl.loop(0, blocks)
    def _(b):
        table[b] = field_v[b].astype(table.dtype)

    copy(incoming, halo, halo_sem).wait()

    @pl.loop(0, blocks)
    def _(b):
        block_product(columns, counts, weights, weights_v, table, total, weights_sem, b)
        wait_rows((rhs, degree), (rhs_v, degree_v), rows_sem, b)
        x, d = field_v[b], degree_v[b]
        left = rhs_v[b] - (d * x - total[...])
        residue[pl.ds(pl.multiple_of(b * size, size), size), :] = left
        base_v[b] = x + DAMPING * left / d
        copy(base_v.at[b], base.at[b], base_sem).start()

    group = 8

    @pl.loop(0, residue.shape[0] // group)
    def _(g):
        start = pl.multiple_of(g * group, group)
        for first in range(0, group, BATCH):
            at = [targets[start + first + k] for k in range(BATCH)]
            held = [coarse[pl.ds(a, 1), :] for a in at]
            sums = []
            for k in range(BATCH):
                old = held[k]
                for j in range(k):
                    old = jnp.where(at[k] == at[j], sums[j], old)
                sums.append(old + residue[pl.ds(start + first + k, 1), :])
            for k in range(BATCH):
                coarse[pl.ds(at[k], 1), :] = sums[k]

    parts = (part0, part1, part2, part3)
    rows = aggregates // len(parts)
    for k in reversed(range(len(parts))):

        @pl.loop(0, rows // chunk)
        def _(i):
            at = pl.ds(pl.multiple_of(k * rows + i * chunk, chunk), chunk)
            coarse_b[at, :] = coarse[at, :].astype(coarse_b.dtype)

        copy(coarse_b.at[pl.ds(k * rows, rows)], parts[k], part_sem.at[k]).start()
    for k in range(len(parts)):
        copy(coarse_b.at[pl.ds(k * rows, rows)], parts[k], part_sem.at[k]).wait()
    copy(base_v, base, base_sem).wait()


def second_step(columns, counts, targets, weights, field, incoming, rhs, degree, aggregates):
    blocks, size, width = field.shape
    slots = weights.shape[1]
    f32, bf16 = jnp.float32, jnp.bfloat16
    part = jax.ShapeDtypeStruct((aggregates // 4, width), bf16)
    return pl.pallas_call(
        second_kernel,
        out_shape=(jax.ShapeDtypeStruct(field.shape, f32), part, part, part, part),
        in_specs=[SMEM] * 3 + [HBM] * 5,
        out_specs=(HBM,) * 5,
        scratch_shapes=[
            pltpu.VMEM(weights.shape, bf16),
            pltpu.VMEM((blocks + incoming.shape[0], size, width), bf16),
            pltpu.VMEM(field.shape, f32),
            pltpu.VMEM(field.shape, f32),
            pltpu.VMEM(field.shape, f32),
            pltpu.VMEM(field.shape, f32),
            pltpu.VMEM((blocks * size, width), f32),
            pltpu.VMEM((aggregates, width), f32),
            pltpu.VMEM((aggregates, width), bf16),
            pltpu.VMEM((size, width), f32),
            pltpu.SemaphoreType.DMA((blocks, slots // HALF)),
            pltpu.SemaphoreType.DMA((blocks, 2)),
            pltpu.SemaphoreType.DMA,
            pltpu.SemaphoreType.DMA,
            pltpu.SemaphoreType.DMA,
            pltpu.SemaphoreType.DMA((4,)),
        ],
        compiler_params=pltpu.CompilerParams(vmem_limit_bytes=VMEM_LIMIT),
        cost_estimate=pl.CostEstimate(
            flops=2 * blocks * slots * size * size * width,
            bytes_accessed=28 << 20, transcendentals=0,
        ),
        name="second",
    )(columns, counts, targets, weights, field, incoming, rhs, degree)


def third_kernel(
    columns, counts, sources, weights, base, degree, part0, part1, part2, part3,
    result,
    weights_v, table, base_v, degree_v, result_v, coarse_b, coarse, picked, total,
    weights_sem, rows_sem, part_sem, result_sem,
):
    blocks, size = base.shape[0], base.shape[1]
    parts = (part0, part1, part2, part3)
    rows = part0.shape[0]
    for k in range(len(parts)):
        copy(parts[k], coarse_b.at[pl.ds(k * rows, rows)], part_sem.at[k]).start()
    load_operands(
        counts, weights, (base, degree), weights_v, (base_v, degree_v), weights_sem, rows_sem
    )
    chunk = 256
    for k in range(len(parts)):
        copy(parts[k], coarse_b.at[pl.ds(k * rows, rows)], part_sem.at[k]).wait()

        @pl.loop(0, rows // chunk)
        def _(i):
            at = pl.ds(pl.multiple_of(k * rows + i * chunk, chunk), chunk)
            coarse[at, :] = coarse_b[at, :].astype(coarse.dtype)

    @pl.loop(0, table.shape[0])
    def _(t):
        for r in range(size):
            picked[pl.ds(r, 1), :] = coarse[pl.ds(sources[t * size + r], 1), :]
        table[t] = picked[...].astype(table.dtype)

    @pl.loop(0, blocks)
    def _(b):
        block_product(columns, counts, weights, weights_v, table, total, weights_sem, b)
        wait_rows((base, degree), (base_v, degree_v), rows_sem, b)
        fix, d = table[b].astype(jnp.float32), degree_v[b]
        result_v[b] = base_v[b] + fix - DAMPING * (d * fix - total[...]) / d
        copy(result_v.at[b], result.at[b], result_sem).start()

    copy(result_v, result, result_sem).wait()


def third_step(columns, counts, sources, weights, base, degree, parts):
    blocks, size, width = base.shape
    slots = weights.shape[1]
    rows = parts[0].shape[0]
    f32, bf16 = jnp.float32, jnp.bfloat16
    return pl.pallas_call(
        third_kernel,
        out_shape=jax.ShapeDtypeStruct(base.shape, f32),
        in_specs=[SMEM] * 3 + [HBM] * 7,
        out_specs=HBM,
        scratch_shapes=[
            pltpu.VMEM(weights.shape, bf16),
            pltpu.VMEM((sources.shape[0] // size, size, width), bf16),
            pltpu.VMEM(base.shape, f32),
            pltpu.VMEM(base.shape, f32),
            pltpu.VMEM(base.shape, f32),
            pltpu.VMEM((4 * rows, width), bf16),
            pltpu.VMEM((4 * rows, width), f32),
            pltpu.VMEM((size, width), f32),
            pltpu.VMEM((size, width), f32),
            pltpu.SemaphoreType.DMA((blocks, slots // HALF)),
            pltpu.SemaphoreType.DMA((blocks, 2)),
            pltpu.SemaphoreType.DMA((4,)),
            pltpu.SemaphoreType.DMA,
        ],
        compiler_params=pltpu.CompilerParams(vmem_limit_bytes=VMEM_LIMIT),
        cost_estimate=pl.CostEstimate(
            flops=2 * blocks * slots * size * size * width,
            bytes_accessed=24 << 20, transcendentals=0,
        ),
        name="third",
    )(columns, counts, sources, weights, base, degree, *parts)


class Stages:
    def __init__(self, mesh):
        n_rows, n_cores = mesh.shape["rows"], mesh.shape["cores"]
        bits = [("rows", 1 << k) for k in range((n_rows - 1).bit_length())]
        inner = [("cores", 1 << k) for k in range((n_cores - 1).bit_length())]
        self.first = bits[0]
        self.orders = (bits[1:] + inner, bits[1:][::-1] + inner)
        self.n_rows, self.n_cores = n_rows, n_cores

    def partner(self, stage):
        axis, bit = stage
        pairs = []
        for r in range(self.n_rows):
            for c in range(self.n_cores):
                other = (r ^ bit, c) if axis == "rows" else (r, c ^ bit)
                pairs.append((r * self.n_cores + c, other[0] * self.n_cores + other[1]))
        return pairs

    def exchange(self, value, stage):
        return lax.ppermute(value, AXES, self.partner(stage))

    def mine(self, stage):
        axis, bit = stage
        return (lax.axis_index(axis) & bit) // bit

    def masks(self, total):
        shared = self.mine(self.first) * (total // 2)
        found = []
        for order in self.orders:
            size, mask = total // 4, shared
            for stage in order:
                size //= 2
                mask = mask + self.mine(stage) * size
            found.append(mask)
        return found

    def relative(self, ids, total):
        low, high = self.masks(total)
        return ids ^ jnp.where((ids & (total // 4)) == 0, low, high)


def add(kept, received):
    return kept.astype(jnp.float32) + received.astype(jnp.float32)


def body(stages, rhs, guess, degree, weights, columns, block_counts, send_lists, aggregates, coarse_diag):
    blocks, slots, size, _ = weights.shape
    width = rhs.shape[1]
    total = coarse_diag.shape[0]
    devices = send_lists.shape[1]
    lists = send_lists.reshape(-1)
    columns = columns.reshape(-1)
    rhs = rhs.reshape(blocks, size, width)
    guess = guess.reshape(blocks, size, width)
    degree = jnp.broadcast_to(degree[:, None], (blocks * size, width)).reshape(blocks, size, width)

    def halo(outgoing):
        shape = outgoing.shape
        outgoing = outgoing.reshape((devices, shape[0] // devices) + shape[1:])
        return lax.all_to_all(
            outgoing, AXES, split_axis=0, concat_axis=0, tiled=True
        ).reshape(shape)

    incoming = halo(pack(lists, guess))
    ids = aggregates.reshape(blocks, size)
    halo_ids = halo(ids[lists])
    all_ids = stages.relative(jnp.concatenate([aggregates, halo_ids.reshape(-1)]), total)
    first, outgoing = first_step(columns, block_counts, lists, weights, guess, incoming, rhs, degree)
    base, *parts = second_step(
        columns, block_counts, all_ids[: aggregates.shape[0]], weights, first, halo(outgoing), rhs, degree, total
    )

    shares = [
        add(parts[k], stages.exchange(parts[2 + k], stages.first)).astype(jnp.bfloat16) for k in range(2)
    ]
    depth = len(stages.orders[0])
    for step in range(depth):
        for k in range(2):
            kept, sent = jnp.split(shares[k], 2)
            summed = add(kept, stages.exchange(sent, stages.orders[k][step]))
            shares[k] = summed if step == depth - 1 else summed.astype(jnp.bfloat16)
    for k, mask in enumerate(stages.masks(total)):
        rows = shares[k].shape[0]
        start = mask + k * (total // 4)
        diag = lax.dynamic_slice_in_dim(coarse_diag, start, rows)
        shares[k] = (shares[k] / diag[:, None]).astype(jnp.bfloat16)
    for step in reversed(range(depth)):
        for k in range(2):
            other = stages.exchange(shares[k], stages.orders[k][step])
            shares[k] = jnp.concatenate([shares[k], other])
    others = [stages.exchange(share, stages.first) for share in shares]
    result = third_step(columns, block_counts, all_ids, weights, base, degree, shares + others)
    return result.reshape(blocks * size, width)


def solution(mesh):
    split = P(AXES)
    return jax.shard_map(
        functools.partial(body, Stages(mesh)),
        mesh=mesh,
        in_specs=(split,) * 8 + (P(),),
        out_specs=split,
        check_vma=False,
    )
```

```python
import functools

import jax
import jax.numpy as jnp
from jax import lax
from jax.experimental import pallas as pl
from jax.experimental.pallas import tpu as pltpu
from jax.sharding import PartitionSpec as P

AXES = ("rows", "cores")
DAMPING = 0.7
HALF = 8
GROUP = 4
AHEAD = 3
PAIRS = 2
SUMS = 2
BATCH = 8
CHUNK = 256
FULL = 61
CODES = 16
RADIX = 256


F32, BF16 = jnp.float32, jnp.bfloat16
HBM = pl.BlockSpec(memory_space=pltpu.HBM)
SMEM = pl.BlockSpec(memory_space=pltpu.SMEM)
VMEM = pl.BlockSpec(memory_space=pltpu.VMEM)
DMA = pltpu.SemaphoreType.DMA


def params(mib):
    return pltpu.CompilerParams(vmem_limit_bytes=mib * 1024 * 1024)


def copy(src, dst, sem):
    return pltpu.make_async_copy(src, dst, sem)


def start_sends(lists, packed, outgoing, sem):
    size = packed.shape[1]

    @pl.loop(0, lists.shape[1])
    def _(p):
        for j in range(lists.shape[2]):
            there = outgoing.at[p, pl.ds(j * size, size)]
            copy(packed.at[lists[0, p, j]], there, sem).start()


def wait_sends(lists, packed, outgoing, sem):
    sent = outgoing.at[:, pl.ds(0, lists.shape[2] * packed.shape[1])]
    copy(sent, sent, sem).wait()


def pack_kernel(
    lists, field, ids, local, outgoing,
    field_v, packed, high, low, code, codes, in_sem, local_sem, code_sem, out_sem,
):
    blocks, size = field.shape[:2]
    listed = lists.shape[2]

    @pl.loop(0, blocks)
    def _(b):
        copy(field.at[b], field_v.at[b], in_sem.at[b]).start()

    high[...] = (ids[...] // RADIX).astype(F32)
    low[...] = (ids[...] % RADIX).astype(F32)
    code[...] = jnp.zeros(code.shape, F32)

    @pl.loop(0, lists.shape[1])
    def _(p):
        for j in range(listed):
            at = pl.ds(lists[0, p, j], 1)
            code[pl.ds(2 * j, 1), :] = high[at, :]
            code[pl.ds(2 * j + 1, 1), :] = low[at, :]
        codes[p] = code[...].astype(BF16)

    codes_copy = copy(codes, outgoing.at[:, pl.ds(listed * size, CODES)], code_sem)
    codes_copy.start()

    @pl.loop(0, blocks)
    def _(b):
        copy(field.at[b], field_v.at[b], in_sem.at[b]).wait()
        packed[b] = field_v[b].astype(BF16)

    start_sends(lists, packed, outgoing, out_sem)
    local_copy = copy(packed, local, local_sem)
    local_copy.start()
    codes_copy.wait()
    wait_sends(lists, packed, outgoing, out_sem)
    local_copy.wait()


def pack(lists, field, ids):
    blocks, size, width = field.shape
    _, peers, listed = lists.shape
    assert 2 * listed <= CODES
    return pl.pallas_call(
        pack_kernel,
        out_shape=(
            jax.ShapeDtypeStruct(field.shape, BF16),
            jax.ShapeDtypeStruct((peers, listed * size + CODES, width), BF16),
        ),
        in_specs=[SMEM, HBM, VMEM],
        out_specs=(HBM, HBM),
        scratch_shapes=[
            pltpu.VMEM(field.shape, F32),
            pltpu.VMEM(field.shape, BF16),
            pltpu.VMEM(ids.shape, F32),
            pltpu.VMEM(ids.shape, F32),
            pltpu.VMEM((CODES, width), F32),
            pltpu.VMEM((peers, CODES, width), BF16),
            DMA((blocks,)),
            DMA,
            DMA,
            DMA,
        ],
        compiler_params=params(FULL),
        name="pack",
    )(lists, field, ids)


def unpack_ids(codes, listed):
    codes = codes[:, : 2 * listed].astype(jnp.int32).reshape(codes.shape[0], listed, 2, -1)
    return (codes[:, :, 0] * RADIX + codes[:, :, 1]).reshape(-1)


def spread_kernel(degree, result):
    size = degree.shape[1]

    @pl.loop(0, degree.shape[0])
    def _(b):
        result[b] = jnp.broadcast_to(degree[pl.ds(b, 1), :], (size, size)).T


def spread(degree, width):
    blocks, size = degree.shape
    assert size == width
    return pl.pallas_call(
        spread_kernel,
        out_shape=jax.ShapeDtypeStruct((blocks, size, width), F32),
        in_specs=[VMEM],
        out_specs=VMEM,
        compiler_params=params(6),
        cost_estimate=pl.CostEstimate(flops=10**10, bytes_accessed=2 << 20, transcendentals=0),
        name="spread",
    )(degree)


class Fetch:
    def __init__(self, counts, order, weights, weights_v, sem, rows=(), rows_v=(), rows_sem=None):
        self.counts, self.order = counts, order
        self.weights, self.weights_v, self.sem = weights, weights_v, sem
        self.rows, self.rows_sem = tuple(zip(rows, rows_v)), rows_sem
        self.blocks, self.slots = weights.shape[0], weights.shape[1]
        self.groups = self.blocks // GROUP

        def place(b, found):
            long = counts[b] > HALF
            order[jnp.where(long, found, self.blocks - 1 - (b - found))] = b
            return found + long.astype(jnp.int32)

        lax.fori_loop(0, self.blocks, place, jnp.int32(0))
        for g in range(AHEAD):
            self.start(g)

    def members(self, g):
        return [self.order[g * GROUP + i] for i in range(GROUP)]

    def each(self, g, act):
        members, slot = self.members(g), g % (AHEAD + 1)

        def halves(h):
            at = pl.ds(h * HALF, HALF)
            for i, b in enumerate(members):
                held = self.weights_v.at[slot, i, at]
                act(copy(self.weights.at[b, at], held, self.sem.at[slot, i, h]))

        halves(0)
        for b in members:
            for k, (src, dst) in enumerate(self.rows):
                act(copy(src.at[b], dst.at[b], self.rows_sem.at[b, k]))
        for h in range(1, self.slots // HALF):

            @pl.when(self.counts[members[0]] > h * HALF)
            def _():
                halves(h)

    def start(self, g):
        self.each(g, lambda one: one.start())

    def product(self, columns, table, g, i, b, h):
        slot = g % (AHEAD + 1)
        left = [self.weights_v[slot, i, h * HALF + s] for s in range(HALF)]
        right = [table[columns[b, h * HALF + s]] for s in range(HALF)]
        return jnp.dot(
            jnp.concatenate(left, 1), jnp.concatenate(right, 0), preferred_element_type=F32
        )

    def sums(self, columns, table, total, g):
        @pl.when(g + AHEAD < self.groups)
        def _():
            self.start(g + AHEAD)

        self.each(g, lambda one: one.wait())
        members = self.members(g)
        for i, b in enumerate(members):
            total[i] = self.product(columns, table, g, i, b, 0)
        for h in range(1, self.slots // HALF):

            @pl.when(self.counts[members[0]] > h * HALF)
            def _():
                for i, b in enumerate(members):
                    more = self.product(columns, table, g, i, b, h)
                    total[i] += jnp.where(self.counts[b] > h * HALF, more, 0.0)

        return members


class Table:
    def __init__(self, table, local, incoming, sem):
        blocks, size, _ = local.shape
        peers = incoming.shape[0]
        listed = (table.shape[0] - blocks) // peers
        self.table, self.incoming, self.sem = table, incoming, sem
        self.blocks, self.size, self.peers, self.listed = blocks, size, peers, listed
        self.local = copy(local, table.at[pl.ds(0, blocks)], sem.at[0])

    def start(self):
        @pl.loop(0, self.peers)
        def _(p):
            for j in range(self.listed):
                block = self.incoming.at[p, pl.ds(j * self.size, self.size)]
                to = self.table.at[self.blocks + p * self.listed + j]
                copy(block, to, self.sem.at[1]).start()

        self.local.start()

    def wait(self):
        halo = self.table.at[pl.ds(self.blocks, self.peers * self.listed)]
        copy(halo, halo, self.sem.at[1]).wait()
        self.local.wait()


def first_kernel(
    columns, counts, lists, weights, local, incoming, field, rhs, degree,
    result, result_b, outgoing,
    order, weights_v, table_v, total, weights_sem, table_sem,
    field_v, rhs_v, degree_v, result_v, packed, rows_sem, result_sem, packed_sem, out_sem,
):
    table = Table(table_v, local, incoming, table_sem)
    table.start()
    fetch = Fetch(
        counts, order, weights, weights_v, weights_sem,
        (field, rhs, degree), (field_v, rhs_v, degree_v), rows_sem,
    )
    table.wait()

    @pl.loop(0, fetch.groups)
    def _(g):
        for i, b in enumerate(fetch.sums(columns, table_v, total, g)):
            x, d = field_v[b], degree_v[b]
            first = x + DAMPING * (rhs_v[b] - (d * x - total[i])) / d
            result_v[b] = first
            packed[b] = first.astype(BF16)
            copy(result_v.at[b], result.at[b], result_sem).start()

    start_sends(lists, packed, outgoing, out_sem)
    packed_copy = copy(packed, result_b, packed_sem)
    packed_copy.start()
    copy(result_v, result, result_sem).wait()
    wait_sends(lists, packed, outgoing, out_sem)
    packed_copy.wait()


def product_cost(weights, width, bytes_accessed):
    blocks, slots, size, _ = weights.shape
    return pl.CostEstimate(
        flops=2 * blocks * slots * size * size * width,
        bytes_accessed=bytes_accessed,
        transcendentals=0,
    )


def product_scratch(weights, tables, width):
    blocks, slots, size, _ = weights.shape
    return [
        pltpu.SMEM((blocks,), jnp.int32),
        pltpu.VMEM((AHEAD + 1, GROUP, slots, size, size), BF16),
        pltpu.VMEM((tables, size, width), BF16),
        pltpu.VMEM((GROUP, size, width), F32),
        DMA((AHEAD + 1, GROUP, slots // HALF)),
    ]


def mib(count, kind):
    return -(-count * jnp.dtype(kind).itemsize // (1 << 20))


def first_step(columns, counts, lists, weights, local, incoming, field, rhs, degree):
    blocks, size, width = field.shape
    _, peers, listed = lists.shape
    tables = blocks + peers * listed
    one = pltpu.VMEM(field.shape, F32)
    return pl.pallas_call(
        first_kernel,
        out_shape=(
            jax.ShapeDtypeStruct(field.shape, F32),
            jax.ShapeDtypeStruct(field.shape, BF16),
            jax.ShapeDtypeStruct((peers, listed * size, width), BF16),
        ),
        in_specs=[SMEM] * 3 + [HBM] * 6,
        out_specs=(HBM,) * 3,
        scratch_shapes=product_scratch(weights, tables, width)
        + [DMA((2,)), one, one, one, one, pltpu.VMEM(field.shape, BF16), DMA((blocks, 3)), DMA, DMA, DMA],
        compiler_params=params(FULL),
        cost_estimate=product_cost(weights, width, 24 << 20),
        name="first",
    )(columns, counts, lists, weights, local, incoming, field, rhs, degree)


def scatter_rows(targets, residue, coarse, b):
    size = residue.shape[1]
    for first in range(0, size, BATCH):
        rows = range(first, first + BATCH)
        at = {r: targets[b * size + r] for r in rows}
        held = {r: coarse[r % SUMS][pl.ds(at[r], 1), :] for r in rows}
        sums = {}
        for r in rows:
            old = held[r]
            for q in range(first + (r - first) % SUMS, r, SUMS):
                old = jnp.where(at[r] == at[q], sums[q], old)
            sums[r] = old + residue[b, pl.ds(r, 1), :]
        for r in rows:
            coarse[r % SUMS][pl.ds(at[r], 1), :] = sums[r]


def second_kernel(
    columns, counts, targets, weights, local, incoming, field, rhs, degree,
    base, part0, part1, part2, part3,
    order, weights_v, table_v, total, weights_sem, table_sem,
    field_v, rhs_v, degree_v, coarse0, coarse1, coarse_b, rows_sem, base_sem, part_sem,
):
    blocks, width = field.shape[0], field.shape[2]
    table = Table(table_v, local, incoming, table_sem)
    table.start()
    fetch = Fetch(
        counts, order, weights, weights_v, weights_sem,
        (field, rhs, degree), (field_v, rhs_v, degree_v), rows_sem,
    )
    coarse = (coarse0, coarse1)
    aggregates = coarse0.shape[0]

    @pl.loop(0, aggregates // CHUNK)
    def _(i):
        for one in coarse:
            one[pl.ds(pl.multiple_of(i * CHUNK, CHUNK), CHUNK), :] = jnp.zeros((CHUNK, width), F32)

    table.wait()

    @pl.loop(0, fetch.groups)
    def _(g):
        for i, b in enumerate(fetch.sums(columns, table_v, total, g)):
            x, d = field_v[b], degree_v[b]
            left = rhs_v[b] - (d * x - total[i])
            rhs_v[b] = left
            field_v[b] = x + DAMPING * left / d
            copy(field_v.at[b], base.at[b], base_sem).start()

    @pl.loop(0, blocks)
    def _(b):
        scatter_rows(targets, rhs_v, coarse, b)

    parts = (part0, part1, part2, part3)
    rows = aggregates // len(parts)
    order_of_use = (2, 3, 0, 1)
    for k in order_of_use:

        @pl.loop(0, rows // CHUNK)
        def _(i):
            at = pl.ds(pl.multiple_of(k * rows + i * CHUNK, CHUNK), CHUNK)
            coarse_b[at, :] = (coarse0[at, :] + coarse1[at, :]).astype(BF16)

        copy(coarse_b.at[pl.ds(k * rows, rows)], parts[k], part_sem.at[k]).start()
    for k in order_of_use:
        copy(coarse_b.at[pl.ds(k * rows, rows)], parts[k], part_sem.at[k]).wait()
    copy(field_v, base, base_sem).wait()


def second_step(columns, counts, targets, weights, local, incoming, field, rhs, degree, tables, aggregates):
    blocks, size, width = field.shape
    part = jax.ShapeDtypeStruct((aggregates // 4, width), BF16)
    one, whole = pltpu.VMEM(field.shape, F32), pltpu.VMEM((aggregates, width), F32)
    return pl.pallas_call(
        second_kernel,
        out_shape=(jax.ShapeDtypeStruct(field.shape, F32), part, part, part, part),
        in_specs=[SMEM] * 3 + [HBM] * 6,
        out_specs=(HBM,) * 5,
        scratch_shapes=product_scratch(weights, tables, width)
        + [DMA((2,)), one, one, one, whole, whole, pltpu.VMEM((aggregates, width), BF16)]
        + [DMA((blocks, 3)), DMA, DMA((4,))],
        compiler_params=params(FULL),
        cost_estimate=product_cost(weights, width, 28 << 20),
        name="second",
    )(columns, counts, targets, weights, local, incoming, field, rhs, degree)


def third_kernel(*refs):
    columns, counts, own_ids, halo_ids, weights, base, degree = refs[:7]
    n_own, n_pair = 4 * PAIRS, 2 * PAIRS
    own, pair, refs = refs[7 : 7 + n_own], refs[7 + n_own : 7 + n_own + n_pair], refs[7 + n_own + n_pair :]
    result, order, weights_v, table, total, sem, coarse, picked = refs
    blocks, size, width = base.shape
    rows = own[0].shape[0]
    fetch = Fetch(counts, order, weights, weights_v, sem)

    pieces = [(one, 0) for one in own]
    for pairs in range(PAIRS):
        for k in range(2):
            pieces += [(one, k * rows) for one in pair[2 * pairs : 2 * pairs + 2]]
    for k, (piece, start) in enumerate(pieces):
        for i in range(rows // CHUNK):
            coarse[pl.ds(k * rows + i * CHUNK, CHUNK), :] = piece[
                pl.ds(start + i * CHUNK, CHUNK), :
            ].astype(F32)

    def gather(ids, start, t):
        for r in range(size):
            picked[pl.ds(r, 1), :] = coarse[pl.ds(ids[t * size + r], 1), :]
        table[start + t] = picked[...].astype(BF16)

    @pl.loop(0, blocks)
    def _(b):
        gather(own_ids, 0, b)

    @pl.loop(0, table.shape[0] - blocks)
    def _(t):
        gather(halo_ids, blocks, t)

    @pl.loop(0, fetch.groups)
    def _(g):
        for i, b in enumerate(fetch.sums(columns, table, total, g)):
            fix, d = table[b].astype(F32), degree[b]
            result[b] = base[b] + fix - DAMPING * (d * fix - total[i]) / d


def third_step(columns, counts, own_ids, halo_ids, weights, base, degree, own, pair):
    blocks, size, width = base.shape
    total = 2 * len(own) * own[0].shape[0]
    tables = (own_ids.shape[0] + halo_ids.shape[0]) // size
    return pl.pallas_call(
        third_kernel,
        out_shape=jax.ShapeDtypeStruct(base.shape, F32),
        in_specs=[SMEM] * 4 + [HBM] + [VMEM] * (2 + len(own) + len(pair)),
        out_specs=VMEM,
        scratch_shapes=product_scratch(weights, tables, width)
        + [pltpu.VMEM((total, width), F32), pltpu.VMEM((size, width), F32)],
        compiler_params=params(31 + mib(tables * size * width, BF16)),
        cost_estimate=product_cost(weights, width, 24 << 20),
        name="third",
    )(columns, counts, own_ids, halo_ids, weights, base, degree, *own, *pair)


class Coarse:
    def __init__(self, mesh, total):
        self.total = total
        self.stream = total // (4 * PAIRS)
        self.n_rows, self.n_cores = mesh.shape["rows"], mesh.shape["cores"]
        bits = [1 << k for k in range((self.n_rows - 1).bit_length())]
        self.pair, self.orders = bits[0], (bits[1:], bits[1:][::-1])

    def exchange(self, value, rows_bit=0, cores_bit=0):
        pairs = []
        for r in range(self.n_rows):
            for c in range(self.n_cores):
                there = (r ^ rows_bit) * self.n_cores + (c ^ cores_bit)
                pairs.append((r * self.n_cores + c, there))
        return lax.ppermute(value, AXES, pairs)

    def masks(self):
        row, core = lax.axis_index("rows"), lax.axis_index("cores")
        found = []
        for order in self.orders:
            size = self.stream
            mask = ((row & self.pair) // self.pair) * (self.total // 2)
            for bit in order:
                size //= 2
                mask = mask + ((row & bit) // bit) * size
            found.append(mask + core * (size // self.n_cores))
        return found

    def place(self, ids):
        low, high = self.masks()
        return ids ^ jnp.where((ids & self.stream) == 0, low, high)

    def reduce(self, parts):
        received = [self.exchange(part, self.pair) for part in parts[PAIRS:]]
        kept = [
            [[one[k * self.stream : (k + 1) * self.stream] for one in both] for k in range(2)]
            for both in zip(parts, received)
        ]
        size = self.stream
        for bits in zip(*self.orders):
            size //= 2
            for pair in kept:
                for k, bit in enumerate(bits):
                    sent = sum(one[size:].astype(F32) for one in pair[k]).astype(BF16)
                    pair[k] = [one[:size] for one in pair[k]] + [self.exchange(sent, bit)]
        size //= self.n_cores

        def share(pair, q):
            return jnp.stack(
                [sum(one[q * size : (q + 1) * size].astype(F32) for one in pair[k]) for k in range(2)]
            )

        totals = []
        for pair in kept:
            received = [
                self.exchange(share(pair, q).astype(BF16), cores_bit=q)
                for q in range(1, self.n_cores)
            ]
            totals.append(share(pair, 0) + sum(one.astype(F32) for one in received))
        return totals

    def diagonal(self, coarse_diag, pair, rows):
        starts = [mask + (2 * pair + k) * self.stream for k, mask in enumerate(self.masks())]
        return jnp.stack([lax.dynamic_slice_in_dim(coarse_diag, start, rows) for start in starts])

    def gather(self, shares):
        held = []
        for share in shares:
            parts = [share] + [self.exchange(share, cores_bit=q) for q in range(1, self.n_cores)]
            held.append([jnp.concatenate([one[k] for one in parts]) for k in range(2)])
        steps = list(zip(*self.orders))[::-1]
        for bits in steps[:-1]:
            for pair in held:
                for k, bit in enumerate(bits):
                    pair[k] = jnp.concatenate([pair[k], self.exchange(pair[k], bit)])
        own, across = [], []
        for pair in held:
            others = [self.exchange(pair[k], bit) for k, bit in enumerate(steps[-1])]
            for k in range(2):
                own += [pair[k], others[k]]
            across += [
                self.exchange(jnp.concatenate(pair), self.pair),
                self.exchange(jnp.concatenate(others), self.pair),
            ]
        return own, across


def body(mesh, rhs, guess, degree, weights, columns, counts, lists, aggregates, coarse_diag):
    blocks, slots, size, _ = weights.shape
    width = rhs.shape[1]
    rhs = rhs.reshape(blocks, size, width)
    guess = guess.reshape(blocks, size, width)
    degree = degree.reshape(blocks, size)
    coarse = Coarse(mesh, coarse_diag.shape[0])

    listed = lists.shape[2] * size

    def halo(outgoing):
        return lax.all_to_all(outgoing, AXES, split_axis=0, concat_axis=0, tiled=True)

    local, outgoing = pack(lists, guess, aggregates.reshape(blocks, size))
    incoming = halo(outgoing)

    degree, own_ids, local = lax.optimization_barrier((degree, aggregates, local))
    own_ids = coarse.place(own_ids)
    degree = spread(degree, width)
    first, first_b, outgoing = first_step(
        columns, counts, lists, weights, local, incoming, guess, rhs, degree
    )
    halo_ids = coarse.place(unpack_ids(incoming[:, listed:], lists.shape[2]))
    base, *parts = second_step(
        columns, counts, own_ids, weights, first_b, halo(outgoing), first, rhs, degree,
        blocks + lists.shape[1] * lists.shape[2], coarse.total,
    )
    shares = []
    for pair, total in enumerate(coarse.reduce(parts)):
        diagonal = coarse.diagonal(coarse_diag, pair, total.shape[1])
        shares.append((total / diagonal[:, :, None]).astype(BF16))
    own, across = coarse.gather(shares)
    result = third_step(columns, counts, own_ids, halo_ids, weights, base, degree, own, across)
    return result.reshape(blocks * size, width)


def solution(mesh):
    split = P(AXES)
    return jax.shard_map(
        functools.partial(body, mesh),
        mesh=mesh,
        in_specs=(split,) * 8 + (P(),),
        out_specs=split,
        check_vma=False,
    )
```

```python
import functools

import jax
import jax.numpy as jnp
from jax import lax
from jax.experimental import pallas as pl
from jax.experimental.pallas import tpu as pltpu
from jax.sharding import PartitionSpec as P

AXES = ("rows", "cores")
DAMPING = 0.7
HALF = 8
GROUP = 4
AHEAD = 3
PAIRS = 2
BATCH = 8
CHUNK = 256
FULL = 61
CODES = 16
RADIX = 256


F32, BF16 = jnp.float32, jnp.bfloat16
HBM = pl.BlockSpec(memory_space=pltpu.HBM)
SMEM = pl.BlockSpec(memory_space=pltpu.SMEM)
VMEM = pl.BlockSpec(memory_space=pltpu.VMEM)
DMA = pltpu.SemaphoreType.DMA


def params(mib):
    return pltpu.CompilerParams(vmem_limit_bytes=mib * 1024 * 1024)


def copy(src, dst, sem):
    return pltpu.make_async_copy(src, dst, sem)


def start_sends(lists, packed, outgoing, sem):
    size = packed.shape[1]

    @pl.loop(0, lists.shape[1])
    def _(p):
        for j in range(lists.shape[2]):
            there = outgoing.at[p, pl.ds(j * size, size)]
            copy(packed.at[lists[0, p, j]], there, sem).start()


def wait_sends(lists, packed, outgoing, sem):
    sent = outgoing.at[:, pl.ds(0, lists.shape[2] * packed.shape[1])]
    copy(sent, sent, sem).wait()


def pack_kernel(
    lists, field, ids, local, outgoing,
    field_v, packed, high, low, code, codes, in_sem, local_sem, code_sem, out_sem,
):
    blocks, size = field.shape[:2]
    listed = lists.shape[2]

    @pl.loop(0, blocks)
    def _(b):
        copy(field.at[b], field_v.at[b], in_sem.at[b]).start()

    high[...] = (ids[...] // RADIX).astype(F32)
    low[...] = (ids[...] % RADIX).astype(F32)
    code[...] = jnp.zeros(code.shape, F32)

    @pl.loop(0, lists.shape[1])
    def _(p):
        for j in range(listed):
            at = pl.ds(lists[0, p, j], 1)
            code[pl.ds(2 * j, 1), :] = high[at, :]
            code[pl.ds(2 * j + 1, 1), :] = low[at, :]
        codes[p] = code[...].astype(BF16)

    codes_copy = copy(codes, outgoing.at[:, pl.ds(listed * size, CODES)], code_sem)
    codes_copy.start()

    @pl.loop(0, blocks)
    def _(b):
        copy(field.at[b], field_v.at[b], in_sem.at[b]).wait()
        packed[b] = field_v[b].astype(BF16)

    start_sends(lists, packed, outgoing, out_sem)
    local_copy = copy(packed, local, local_sem)
    local_copy.start()
    codes_copy.wait()
    wait_sends(lists, packed, outgoing, out_sem)
    local_copy.wait()


def pack(lists, field, ids):
    blocks, size, width = field.shape
    _, peers, listed = lists.shape
    assert 2 * listed <= CODES
    return pl.pallas_call(
        pack_kernel,
        out_shape=(
            jax.ShapeDtypeStruct(field.shape, BF16),
            jax.ShapeDtypeStruct((peers, listed * size + CODES, width), BF16),
        ),
        in_specs=[SMEM, HBM, VMEM],
        out_specs=(HBM, HBM),
        scratch_shapes=[
            pltpu.VMEM(field.shape, F32),
            pltpu.VMEM(field.shape, BF16),
            pltpu.VMEM(ids.shape, F32),
            pltpu.VMEM(ids.shape, F32),
            pltpu.VMEM((CODES, width), F32),
            pltpu.VMEM((peers, CODES, width), BF16),
            DMA((blocks,)),
            DMA,
            DMA,
            DMA,
        ],
        compiler_params=params(FULL),
        name="pack",
    )(lists, field, ids)


def unpack_ids(codes, listed):
    codes = codes[:, : 2 * listed].astype(jnp.int32).reshape(codes.shape[0], listed, 2, -1)
    return (codes[:, :, 0] * RADIX + codes[:, :, 1]).reshape(-1)


def spread_kernel(degree, result):
    size = degree.shape[1]

    @pl.loop(0, degree.shape[0])
    def _(b):
        result[b] = jnp.broadcast_to(degree[pl.ds(b, 1), :], (size, size)).T


def spread(degree, width):
    blocks, size = degree.shape
    assert size == width
    return pl.pallas_call(
        spread_kernel,
        out_shape=jax.ShapeDtypeStruct((blocks, size, width), F32),
        in_specs=[VMEM],
        out_specs=VMEM,
        compiler_params=params(6),
        cost_estimate=pl.CostEstimate(flops=10**10, bytes_accessed=2 << 20, transcendentals=0),
        name="spread",
    )(degree)


class Fetch:
    def __init__(self, counts, order, weights, weights_v, sem, rows=(), rows_v=(), rows_sem=None):
        self.counts, self.order = counts, order
        self.weights, self.weights_v, self.sem = weights, weights_v, sem
        self.rows, self.rows_sem = tuple(zip(rows, rows_v)), rows_sem
        self.blocks, self.slots = weights.shape[0], weights.shape[1]
        self.groups = self.blocks // GROUP

        def place(b, found):
            long = counts[b] > HALF
            order[jnp.where(long, found, self.blocks - 1 - (b - found))] = b
            return found + long.astype(jnp.int32)

        lax.fori_loop(0, self.blocks, place, jnp.int32(0))
        for g in range(AHEAD):
            self.start(g)

    def members(self, g):
        return [self.order[g * GROUP + i] for i in range(GROUP)]

    def each(self, g, act):
        members, slot = self.members(g), g % (AHEAD + 1)

        def halves(h):
            at = pl.ds(h * HALF, HALF)
            for i, b in enumerate(members):
                held = self.weights_v.at[slot, i, at]
                act(copy(self.weights.at[b, at], held, self.sem.at[slot, i, h]))

        halves(0)
        for b in members:
            for k, (src, dst) in enumerate(self.rows):
                act(copy(src.at[b], dst.at[b], self.rows_sem.at[b, k]))
        for h in range(1, self.slots // HALF):

            @pl.when(self.counts[members[0]] > h * HALF)
            def _():
                halves(h)

    def start(self, g):
        self.each(g, lambda one: one.start())

    def product(self, columns, table, g, i, b, h):
        slot = g % (AHEAD + 1)
        left = [self.weights_v[slot, i, h * HALF + s] for s in range(HALF)]
        right = [table[columns[b, h * HALF + s]] for s in range(HALF)]
        return jnp.dot(
            jnp.concatenate(left, 1), jnp.concatenate(right, 0), preferred_element_type=F32
        )

    def sums(self, columns, table, total, g):
        @pl.when(g + AHEAD < self.groups)
        def _():
            self.start(g + AHEAD)

        self.each(g, lambda one: one.wait())
        members = self.members(g)
        for i, b in enumerate(members):
            total[i] = self.product(columns, table, g, i, b, 0)
        for h in range(1, self.slots // HALF):

            @pl.when(self.counts[members[0]] > h * HALF)
            def _():
                for i, b in enumerate(members):
                    more = self.product(columns, table, g, i, b, h)
                    total[i] += jnp.where(self.counts[b] > h * HALF, more, 0.0)

        return members


class Table:
    def __init__(self, table, local, sem):
        self.table, self.blocks = table, local.shape[0]
        self.local = copy(local, table.at[pl.ds(0, self.blocks)], sem)
        self.local.start()

    def fill(self, incoming):
        peers, size = incoming.shape[0], self.table.shape[1]
        listed = (self.table.shape[0] - self.blocks) // peers

        @pl.loop(0, peers)
        def _(p):
            for j in range(listed):
                self.table[self.blocks + p * listed + j] = incoming[p, pl.ds(j * size, size)]

        self.local.wait()


def first_kernel(
    columns, counts, lists, weights, local, incoming, field, rhs, degree,
    result, result_b, outgoing,
    order, weights_v, table_v, total, weights_sem, table_sem,
    field_v, rhs_v, degree_v, result_v, packed, rows_sem, result_sem, packed_sem, out_sem,
):
    table = Table(table_v, local, table_sem)
    fetch = Fetch(
        counts, order, weights, weights_v, weights_sem,
        (field, rhs, degree), (field_v, rhs_v, degree_v), rows_sem,
    )
    table.fill(incoming)

    @pl.loop(0, fetch.groups)
    def _(g):
        for i, b in enumerate(fetch.sums(columns, table_v, total, g)):
            x, d = field_v[b], degree_v[b]
            first = x + DAMPING * (rhs_v[b] - (d * x - total[i])) / d
            result_v[b] = first
            packed[b] = first.astype(BF16)
            copy(result_v.at[b], result.at[b], result_sem).start()

    start_sends(lists, packed, outgoing, out_sem)
    packed_copy = copy(packed, result_b, packed_sem)
    packed_copy.start()
    copy(result_v, result, result_sem).wait()
    wait_sends(lists, packed, outgoing, out_sem)
    packed_copy.wait()


def product_cost(weights, width, bytes_accessed):
    blocks, slots, size, _ = weights.shape
    return pl.CostEstimate(
        flops=2 * blocks * slots * size * size * width,
        bytes_accessed=bytes_accessed,
        transcendentals=0,
    )


def product_scratch(weights, tables, width):
    blocks, slots, size, _ = weights.shape
    return [
        pltpu.SMEM((blocks,), jnp.int32),
        pltpu.VMEM((AHEAD + 1, GROUP, slots, size, size), BF16),
        pltpu.VMEM((tables, size, width), BF16),
        pltpu.VMEM((GROUP, size, width), F32),
        DMA((AHEAD + 1, GROUP, slots // HALF)),
    ]


def mib(count, kind):
    return -(-count * jnp.dtype(kind).itemsize // (1 << 20))


def first_step(columns, counts, lists, weights, local, incoming, field, rhs, degree):
    blocks, size, width = field.shape
    _, peers, listed = lists.shape
    tables = blocks + peers * listed
    one = pltpu.VMEM(field.shape, F32)
    return pl.pallas_call(
        first_kernel,
        out_shape=(
            jax.ShapeDtypeStruct(field.shape, F32),
            jax.ShapeDtypeStruct(field.shape, BF16),
            jax.ShapeDtypeStruct((peers, listed * size, width), BF16),
        ),
        in_specs=[SMEM] * 3 + [HBM, HBM, VMEM] + [HBM] * 3,
        out_specs=(HBM,) * 3,
        scratch_shapes=product_scratch(weights, tables, width)
        + [DMA, one, one, one, one, pltpu.VMEM(field.shape, BF16), DMA((blocks, 3)), DMA, DMA, DMA],
        compiler_params=params(FULL),
        cost_estimate=product_cost(weights, width, 24 << 20),
        name="first",
    )(columns, counts, lists, weights, local, incoming, field, rhs, degree)


def scatter_rows(targets, residue, coarse, b):
    size, sums_of = residue.shape[1], len(coarse)
    for first in range(0, size, BATCH):
        rows = range(first, first + BATCH)
        at = {r: targets[b * size + r] for r in rows}
        held = {r: coarse[r % sums_of][pl.ds(at[r], 1), :] for r in rows}
        sums = {}
        for r in rows:
            old = held[r]
            for q in range(first + (r - first) % sums_of, r, sums_of):
                old = jnp.where(at[r] == at[q], sums[q], old)
            sums[r] = old + residue[b, pl.ds(r, 1), :]
        for r in rows:
            coarse[r % sums_of][pl.ds(at[r], 1), :] = sums[r]


def second_kernel(
    columns, counts, targets, weights, local, incoming, field, rhs, degree,
    base, part0, part1, part2, part3,
    order, weights_v, table_v, total, weights_sem, table_sem,
    field_v, rhs_v, degree_v, coarse_b, rows_sem, base_sem, part_sem,
    *coarse,
):
    blocks, width = field.shape[0], field.shape[2]
    table = Table(table_v, local, table_sem)
    fetch = Fetch(
        counts, order, weights, weights_v, weights_sem,
        (field, rhs, degree), (field_v, rhs_v, degree_v), rows_sem,
    )
    aggregates = coarse[0].shape[0]

    @pl.loop(0, aggregates // CHUNK)
    def _(i):
        for one in coarse:
            one[pl.ds(pl.multiple_of(i * CHUNK, CHUNK), CHUNK), :] = jnp.zeros((CHUNK, width), F32)

    table.fill(incoming)

    @pl.loop(0, fetch.groups)
    def _(g):
        for i, b in enumerate(fetch.sums(columns, table_v, total, g)):
            x, d = field_v[b], degree_v[b]
            left = rhs_v[b] - (d * x - total[i])
            rhs_v[b] = left
            field_v[b] = x + DAMPING * left / d
            copy(field_v.at[b], base.at[b], base_sem).start()

    @pl.loop(0, blocks)
    def _(b):
        scatter_rows(targets, rhs_v, coarse, b)

    parts = (part0, part1, part2, part3)
    rows = aggregates // len(parts)
    order_of_use = (2, 3, 0, 1)
    for k in order_of_use:

        @pl.loop(0, rows // CHUNK)
        def _(i):
            at = pl.ds(pl.multiple_of(k * rows + i * CHUNK, CHUNK), CHUNK)
            coarse_b[at, :] = sum(one[at, :] for one in coarse).astype(BF16)

        copy(coarse_b.at[pl.ds(k * rows, rows)], parts[k], part_sem.at[k]).start()
    for k in order_of_use:
        copy(coarse_b.at[pl.ds(k * rows, rows)], parts[k], part_sem.at[k]).wait()
    copy(field_v, base, base_sem).wait()


def second_step(columns, counts, targets, weights, local, incoming, field, rhs, degree, tables, aggregates):
    blocks, size, width = field.shape
    part = jax.ShapeDtypeStruct((aggregates // 4, width), BF16)
    one, whole = pltpu.VMEM(field.shape, F32), pltpu.VMEM((aggregates, width), F32)
    ring = mib((AHEAD + 1) * GROUP * weights.shape[1] * size * size, BF16)
    held = ring + mib(tables * size * width + incoming.size, BF16)
    held += mib(3 * field.size, F32) + mib(aggregates * width, BF16) + 1
    each = mib(aggregates * width, F32)
    sums = 4 if held + 4 * each < FULL else 2
    return pl.pallas_call(
        second_kernel,
        out_shape=(jax.ShapeDtypeStruct(field.shape, F32), part, part, part, part),
        in_specs=[SMEM] * 3 + [HBM, HBM, VMEM] + [HBM] * 3,
        out_specs=(HBM,) * 5,
        scratch_shapes=product_scratch(weights, tables, width)
        + [DMA, one, one, one, pltpu.VMEM((aggregates, width), BF16)]
        + [DMA((blocks, 3)), DMA, DMA((4,))]
        + [whole] * sums,
        compiler_params=params(FULL),
        cost_estimate=product_cost(weights, width, 28 << 20),
        name="second",
    )(columns, counts, targets, weights, local, incoming, field, rhs, degree)


def third_kernel(*refs):
    columns, counts, own_ids, halo_ids, weights, base, degree = refs[:7]
    n_own, n_pair = 4 * PAIRS, 2 * PAIRS
    own, pair, refs = refs[7 : 7 + n_own], refs[7 + n_own : 7 + n_own + n_pair], refs[7 + n_own + n_pair :]
    result, order, weights_v, table, total, sem, coarse, picked = refs
    blocks, size, width = base.shape
    rows = own[0].shape[0]
    fetch = Fetch(counts, order, weights, weights_v, sem)

    pieces = [(one, 0) for one in own]
    for pairs in range(PAIRS):
        for k in range(2):
            pieces += [(one, k * rows) for one in pair[2 * pairs : 2 * pairs + 2]]
    for k, (piece, start) in enumerate(pieces):
        for i in range(rows // CHUNK):
            coarse[pl.ds(k * rows + i * CHUNK, CHUNK), :] = piece[
                pl.ds(start + i * CHUNK, CHUNK), :
            ].astype(F32)

    def gather(ids, start, t):
        for r in range(size):
            picked[pl.ds(r, 1), :] = coarse[pl.ds(ids[t * size + r], 1), :]
        table[start + t] = picked[...].astype(BF16)

    @pl.loop(0, blocks)
    def _(b):
        gather(own_ids, 0, b)

    @pl.loop(0, table.shape[0] - blocks)
    def _(t):
        gather(halo_ids, blocks, t)

    @pl.loop(0, fetch.groups)
    def _(g):
        for i, b in enumerate(fetch.sums(columns, table, total, g)):
            fix, d = table[b].astype(F32), degree[b]
            result[b] = base[b] + fix - DAMPING * (d * fix - total[i]) / d


def third_step(columns, counts, own_ids, halo_ids, weights, base, degree, own, pair):
    blocks, size, width = base.shape
    total = 2 * len(own) * own[0].shape[0]
    tables = (own_ids.shape[0] + halo_ids.shape[0]) // size
    return pl.pallas_call(
        third_kernel,
        out_shape=jax.ShapeDtypeStruct(base.shape, F32),
        in_specs=[SMEM] * 4 + [HBM] + [VMEM] * (2 + len(own) + len(pair)),
        out_specs=VMEM,
        scratch_shapes=product_scratch(weights, tables, width)
        + [pltpu.VMEM((total, width), F32), pltpu.VMEM((size, width), F32)],
        compiler_params=params(31 + mib(tables * size * width, BF16)),
        cost_estimate=product_cost(weights, width, 24 << 20),
        name="third",
    )(columns, counts, own_ids, halo_ids, weights, base, degree, *own, *pair)


class Coarse:
    def __init__(self, mesh, total):
        self.total = total
        self.stream = total // (4 * PAIRS)
        self.n_rows, self.n_cores = mesh.shape["rows"], mesh.shape["cores"]
        bits = [1 << k for k in range((self.n_rows - 1).bit_length())]
        self.pair, self.orders = bits[0], (bits[1:], bits[1:][::-1])

    def exchange(self, value, rows_bit=0, cores_bit=0):
        pairs = []
        for r in range(self.n_rows):
            for c in range(self.n_cores):
                there = (r ^ rows_bit) * self.n_cores + (c ^ cores_bit)
                pairs.append((r * self.n_cores + c, there))
        return lax.ppermute(value, AXES, pairs)

    def masks(self):
        row, core = lax.axis_index("rows"), lax.axis_index("cores")
        found = []
        for order in self.orders:
            size = self.stream
            mask = ((row & self.pair) // self.pair) * (self.total // 2)
            for bit in order:
                size //= 2
                mask = mask + ((row & bit) // bit) * size
            found.append(mask + core * (size // self.n_cores))
        return found

    def place(self, ids):
        low, high = self.masks()
        return ids ^ jnp.where((ids & self.stream) == 0, low, high)

    def reduce(self, parts):
        received = [self.exchange(part, self.pair) for part in parts[PAIRS:]]
        kept = [
            [[one[k * self.stream : (k + 1) * self.stream] for one in both] for k in range(2)]
            for both in zip(parts, received)
        ]
        size = self.stream
        for bits in zip(*self.orders):
            size //= 2
            for pair in kept:
                for k, bit in enumerate(bits):
                    sent = sum(one[size:].astype(F32) for one in pair[k]).astype(BF16)
                    pair[k] = [one[:size] for one in pair[k]] + [self.exchange(sent, bit)]
        size //= self.n_cores

        def share(pair, q):
            return jnp.stack(
                [sum(one[q * size : (q + 1) * size].astype(F32) for one in pair[k]) for k in range(2)]
            )

        totals = []
        for pair in kept:
            received = [
                self.exchange(share(pair, q).astype(BF16), cores_bit=q)
                for q in range(1, self.n_cores)
            ]
            totals.append(share(pair, 0) + sum(one.astype(F32) for one in received))
        return totals

    def diagonal(self, coarse_diag, pair, rows):
        starts = [mask + (2 * pair + k) * self.stream for k, mask in enumerate(self.masks())]
        return jnp.stack([lax.dynamic_slice_in_dim(coarse_diag, start, rows) for start in starts])

    def gather(self, shares):
        held = []
        for share in shares:
            parts = [share] + [self.exchange(share, cores_bit=q) for q in range(1, self.n_cores)]
            held.append([jnp.concatenate([one[k] for one in parts]) for k in range(2)])
        steps = list(zip(*self.orders))[::-1]
        for bits in steps[:-1]:
            for pair in held:
                for k, bit in enumerate(bits):
                    pair[k] = jnp.concatenate([pair[k], self.exchange(pair[k], bit)])
        own, across = [], []
        for pair in held:
            others = [self.exchange(pair[k], bit) for k, bit in enumerate(steps[-1])]
            for k in range(2):
                own += [pair[k], others[k]]
            across += [
                self.exchange(jnp.concatenate(pair), self.pair),
                self.exchange(jnp.concatenate(others), self.pair),
            ]
        return own, across


def body(mesh, rhs, guess, degree, weights, columns, counts, lists, aggregates, coarse_diag):
    blocks, slots, size, _ = weights.shape
    width = rhs.shape[1]
    rhs = rhs.reshape(blocks, size, width)
    guess = guess.reshape(blocks, size, width)
    degree = degree.reshape(blocks, size)
    coarse = Coarse(mesh, coarse_diag.shape[0])

    listed = lists.shape[2] * size

    def halo(outgoing):
        return lax.all_to_all(outgoing, AXES, split_axis=0, concat_axis=0, tiled=True)

    local, outgoing = pack(lists, guess, aggregates.reshape(blocks, size))
    incoming = halo(outgoing)

    degree, own_ids, local = lax.optimization_barrier((degree, aggregates, local))
    own_ids = coarse.place(own_ids)
    degree = spread(degree, width)
    first, first_b, outgoing = first_step(
        columns, counts, lists, weights, local, incoming, guess, rhs, degree
    )
    halo_ids = coarse.place(unpack_ids(incoming[:, listed:], lists.shape[2]))
    base, *parts = second_step(
        columns, counts, own_ids, weights, first_b, halo(outgoing), first, rhs, degree,
        blocks + lists.shape[1] * lists.shape[2], coarse.total,
    )
    shares = []
    for pair, total in enumerate(coarse.reduce(parts)):
        diagonal = coarse.diagonal(coarse_diag, pair, total.shape[1])
        shares.append((total / diagonal[:, :, None]).astype(BF16))
    own, across = coarse.gather(shares)
    result = third_step(columns, counts, own_ids, halo_ids, weights, base, degree, own, across)
    return result.reshape(blocks * size, width)


def solution(mesh):
    split = P(AXES)
    return jax.shard_map(
        functools.partial(body, mesh),
        mesh=mesh,
        in_specs=(split,) * 8 + (P(),),
        out_specs=split,
        check_vma=False,
    )
```
